128 devices in a mesh: row: 8 (over z_lo, x), col: 16 (over y, z_hi, core).
Axes of the slice: x: 4, y: 4, z: 4 (z_hi: 2, z_lo: 2; z = z_hi * 2 + z_lo), core: 2. Of those that a mesh axis runs over, the one named last changes fastest.
Arguments:
- gate_weight: bfloat16 [4608, 36864], P('row', 'col'), may hold values from -8.838835 to 8.838835
- up_weight: bfloat16 [4608, 36864], P('row', 'col'), may hold values from -8.838835 to 8.838835
- routes: int32 [2, 8], replicated, may hold values from 0 to 7, each once within a row
Outputs:
- gate_serving: bfloat16 [4608, 36864], P('col', 'row')
- up_serving: bfloat16 [4608, 36864], P('col', 'row')
- scales: float32 [2, 36864], P(None, 'row')
The draws below stay inside these ranges and needn't reach their ends.
Inputs may be any that keep to these rules, and one draw needn't show every extreme that they name: Each row of routes names every serving rank's piece once.
All inputs are finite; a program needn't handle non-finite values. Where the reference program divides by a largest or mean magnitude, that divisor is 1e-20 or more.
Results may differ from the reference program's by a relative error of at most 0.001.
Values may be sent and summed in bfloat16 or wider, within the bound.
No kernel may reach another device: no remote copies, remote signals or barrier semaphores. Data moves between devices by JAX's collectives and lax.ppermute only.
A program may use at most 64 MiB of HBM per device.

```python
import math
import jax
import jax.numpy as jnp

D = 4608
FF = 36864
SERVE_TP = 8
N_ROW = 8
N_COL = 16


def scaled_weight(key, salt):
    base_key = jax.random.fold_in(key, salt)
    first, second, third = jax.random.split(base_key, 3)
    row_scale = jnp.exp(jax.random.uniform(first, (D, 1), jnp.float32, 0.0, math.log(10.0)))
    col_scale = jnp.exp(jax.random.uniform(second, (1, FF), jnp.float32, 0.0, math.log(10.0)))
    noise = jnp.clip(jax.random.normal(third, (D, FF), jnp.float32), -6.0, 6.0)
    values = noise * row_scale * col_scale / math.sqrt(D)
    return values.astype(jnp.bfloat16)


def draw_gate_weight(key, part):
    return scaled_weight(key, 11)


def draw_up_weight(key, part):
    return scaled_weight(key, 23)


def setup_inputs(seed: int = 0) -> dict:
    keys = jax.random.split(jax.random.key(seed), 4)
    return {
        "gate_weight": draw_gate_weight(jax.random.fold_in(keys[3], 71), 0),
        "up_weight": draw_up_weight(jax.random.fold_in(keys[3], 71), 0),
        "routes": jax.vmap(lambda own: jax.random.permutation(own, SERVE_TP))(jax.random.split(keys[2], 2)).reshape((2, SERVE_TP)).astype(jnp.int32),
    }


EPSILON = 1e-6
LIMIT = 4.0


def convert(weight, order):
    block_len = FF // (N_ROW * N_COL)
    peaks = jnp.max(jnp.abs(weight), axis=0).astype(jnp.float32)
    factor = LIMIT / (peaks + EPSILON)
    quant = (weight.astype(jnp.float32) * factor[None, :]).astype(jnp.bfloat16)
    shaped = quant.reshape(D, N_COL, N_ROW, block_len)
    chosen = jnp.take(shaped, order, axis=2).transpose(0, 2, 1, 3).reshape(D, FF)
    scale_table = ((peaks + EPSILON) / LIMIT).reshape(N_COL, N_ROW, block_len)
    scale_line = jnp.take(scale_table, order, axis=1).transpose(1, 0, 2).reshape(FF)
    return chosen, scale_line


def reference(gate_weight, up_weight, routes):
    gate_serving, gate_scale = convert(gate_weight, routes[0])
    up_serving, up_scale = convert(up_weight, routes[1])
    return gate_serving, up_serving, jnp.stack([gate_scale, up_scale])
```

```python
import itertools

import jax
import jax.numpy as jnp
from jax import lax
from jax.experimental import pallas as pl
from jax.experimental.pallas import tpu as pltpu
from jax.sharding import Mesh
from jax.sharding import PartitionSpec as P


EPSILON = 1e-06
LIMIT = 4.0

ROW = ("zl", "x")
COL = ("y", "zh", "k")
ALL = ROW + COL

L = 288
PIECES = 8
GROUPS = ((0, 80), (80, 80), (160, 64), (224, 64))
DENSE = 2 * L + 80

SMEM = pl.BlockSpec(memory_space=pltpu.SMEM)


def moves(fn):
    index = lambda x, y, zh, zl, k: (((zl * 4 + x) * 4 + y) * 2 + zh) * 2 + k
    every = itertools.product(range(4), range(4), range(2), range(2), range(2))
    return [(index(*c), index(*fn(*c))) for c in every]


def shift_x(value, d):
    return lax.ppermute(value, ALL, moves(lambda x, y, zh, zl, k: (x ^ d, y, zh, zl, k)))


def shift_y(value, d):
    return lax.ppermute(value, ALL, moves(lambda x, y, zh, zl, k: (x, y ^ d, zh, zl, k)))


def shift_z(value, dh, dl):
    return lax.ppermute(value, ALL, moves(lambda x, y, zh, zl, k: (x, y, zh ^ dh, zl ^ dl, k)))


def swap_core(value):
    return lax.ppermute(value, ALL, moves(lambda x, y, zh, zl, k: (x, y, zh, zl, 1 - k)))


def params(mib=24):
    return pltpu.CompilerParams(vmem_limit_bytes=mib * 1024 * 1024)


BLOCK = jax.ShapeDtypeStruct((2, DENSE, 128), jnp.bfloat16)
PAIR = jax.ShapeDtypeStruct((2, 2, DENSE, 128), jnp.bfloat16)


def maxima_kernel(routes_ref, gate_ref, up_ref, out_ref, acc):
    step = pl.program_id(0)
    for p, ref in enumerate((gate_ref, up_ref)):
        part = jnp.max(jnp.abs(ref[...].astype(jnp.float32)), axis=0, keepdims=True)
        acc[p] = jnp.where(step == 0, part, jnp.maximum(acc[p], part))

    @pl.when(step == pl.num_programs(0) - 1)
    def _():
        for p in range(2):
            for r in range(PIECES):
                piece = routes_ref[p, r]
                total = jnp.zeros((1, L), jnp.float32)
                for q in range(PIECES):
                    total = jnp.where(piece == q, acc[p, :, q * L : (q + 1) * L], total)
                out_ref[r, p] = total


def maxima(routes, gate, up):
    rows = 144
    spec = pl.BlockSpec((rows, gate.shape[1]), lambda i: (i, 0))
    return pl.pallas_call(
        maxima_kernel,
        grid=(gate.shape[0] // rows,),
        in_specs=[SMEM, spec, spec],
        out_specs=pl.BlockSpec((PIECES, 2, 1, L), lambda i: (0, 0, 0, 0)),
        out_shape=jax.ShapeDtypeStruct((PIECES, 2, 1, L), jnp.float32),
        scratch_shapes=[pltpu.VMEM((2, 1, gate.shape[1]), jnp.float32)],
        compiler_params=params(),
    )(routes, gate, up)


def pack_kernel(pick_ref, mine_ref, other_ref, *refs):
    outs, held = refs[:-1], refs[-1]
    core = pick_ref[8]
    for which, ref in ((0, mine_ref), (1, other_ref)):
        source = core ^ which
        for q in range(PIECES):
            at = q * L
            held[q, source, 0:L] = ref[:, at : at + 128]
            held[q, source, L : 2 * L] = ref[:, at + 128 : at + 256]
            tail = ref[:, at + 256 : at + L]
            parts = []
            for start, size in GROUPS:
                part = tail[start : start + size]
                if size < 80:
                    part = jnp.concatenate([part, tail[0 : 80 - size]], axis=0)
                parts.append(part)
            held[q, source, 2 * L : DENSE] = jnp.concatenate(parts, axis=1)
    for s, out in enumerate(outs):
        out[...] = held[pick_ref[s]]


def pack(pick, mine, other):
    width = mine.shape[1]
    block = pl.BlockSpec((L, width), lambda i, pick: (pick[8], 0))
    return pl.pallas_call(
        pack_kernel,
        grid_spec=pltpu.PrefetchScalarGridSpec(
            num_scalar_prefetch=1,
            grid=(1,),
            in_specs=[block, block],
            out_specs=[pl.BlockSpec(BLOCK.shape, lambda i, pick: (0, 0, 0))] * PIECES,
            scratch_shapes=[pltpu.VMEM((PIECES, *BLOCK.shape), jnp.bfloat16)],
        ),
        out_shape=[BLOCK] * PIECES,
        compiler_params=params(),
    )(pick, mine, other)


def first_kernel(bits_ref, b0, b1, b2, b3, low, high):
    refs = (b0, b1, b2, b3)
    for a in range(2):
        for b in range(2):

            @pl.when((bits_ref[0] == a) & (bits_ref[1] == b))
            def _(a=a, b=b):
                for f in range(2):
                    low[f] = refs[(f ^ a) * 2 + b][...]
                    high[f] = refs[(f ^ a) * 2 + (1 ^ b)][...]


def first(bits, blocks):
    whole = pl.BlockSpec(memory_space=pltpu.VMEM)
    return pl.pallas_call(
        first_kernel,
        in_specs=[SMEM] + [whole] * 4,
        out_specs=[whole] * 2,
        out_shape=[PAIR] * 2,
        compiler_params=params(),
    )(bits, *blocks)


def second_kernel(bits_ref, c0, c1, *outs):
    refs = (c0, c1)
    for a in range(2):

        @pl.when(bits_ref[2] == a)
        def _(a=a):
            for e in range(2):
                for f in range(2):
                    outs[e * 2 + f][...] = refs[e ^ a][f]


def second(bits, blocks):
    whole = pl.BlockSpec(memory_space=pltpu.VMEM)
    return pl.pallas_call(
        second_kernel,
        in_specs=[SMEM] + [whole] * 2,
        out_specs=[whole] * 4,
        out_shape=[BLOCK] * 4,
        compiler_params=params(),
    )(bits, *blocks)


def unpack_kernel(bits_ref, factor_ref, *refs):
    blocks, out, held = refs[:-2], refs[-2], refs[-1]
    y, zh = bits_ref[3], bits_ref[4]
    for b in range(2):
        for d in range(4):
            held[y ^ d, zh ^ b] = blocks[b * 4 + d][...]
    for y in range(4):
        for j, (start, size) in enumerate(GROUPS):
            lanes = []
            for zh in range(2):
                for k in range(2):
                    for at in (start, L + start):
                        lanes.append(held[y, zh, k, at : at + size].astype(jnp.float32))
                    tail = held[y, zh, k, 2 * L : 2 * L + size].astype(jnp.float32)
                    lanes.append(tail[:, 32 * j : 32 * j + 32])
            at = y * 4 * L
            value = jnp.concatenate(lanes, axis=1) * factor_ref[:, at : at + 4 * L]
            out[start : start + size, at : at + 4 * L] = value.astype(jnp.bfloat16)


def unpack(bits, factor, blocks):
    whole = pl.BlockSpec(memory_space=pltpu.VMEM)
    return pl.pallas_call(
        unpack_kernel,
        in_specs=[SMEM] + [whole] * 9,
        out_specs=whole,
        out_shape=jax.ShapeDtypeStruct((L, 16 * L), jnp.bfloat16),
        scratch_shapes=[pltpu.VMEM((4, 2, *BLOCK.shape), jnp.bfloat16)],
        compiler_params=params(),
    )(bits, factor, *blocks)


def shards(gate, up, routes):
    x, y, zh, zl, k = (lax.axis_index(n) for n in ("x", "y", "zh", "zl", "k"))
    bits = jnp.stack(
        [(x >> 1) ^ (y & 1), (x & 1) ^ zh, zl ^ (y >> 1), y, zh, k, k, k]
    ).astype(jnp.int32)
    slots = jnp.arange(8)
    ranks = (zl ^ (slots >> 2)) * 4 + (x ^ (slots & 3))
    one_hot = (ranks[:, None] == jnp.arange(8)[None, :]).astype(jnp.int32)
    picks = jnp.sum(one_hot[None] * routes[:, None, :], axis=2)
    picks = jnp.concatenate([picks, jnp.full((2, 8), k, jnp.int32)], axis=1)

    others = [swap_core(gate), swap_core(up)]
    local = maxima(routes, gate, up)
    shared = jnp.max(lax.all_to_all(local, ROW, 0, 0, tiled=True), axis=0)
    everyone = lax.all_to_all(
        jnp.broadcast_to(shared[None], (16, *shared.shape)), COL, 0, 0, tiled=True
    )
    peaks = everyone.reshape(16, 2, L).transpose(1, 0, 2).reshape(2, 16 * L)
    scales = (peaks + EPSILON) / LIMIT
    factors = LIMIT / (peaks + EPSILON)

    outs = []
    for p, weight in enumerate((gate, up)):
        blocks = pack(picks[p], weight, others[p])
        pairs = {}
        for c in (1, 0):
            four = blocks[c * 4 : c * 4 + 4]
            four = [four[0]] + [shift_x(four[d], d) for d in (1, 2, 3)]
            low, high = first(bits, four)
            pairs[0, c] = shift_z(low, 0, 1) if c else low
            pairs[1, c] = shift_z(high, 1, c)
        final = []
        for b in range(2):
            four = second(bits, (pairs[b, 0], pairs[b, 1]))
            final += [four[0]] + [shift_y(four[d], d) for d in (1, 2, 3)]
        outs.append(unpack(bits, factors[p : p + 1], final))
    return outs[0], outs[1], scales


def solution(mesh):
    finer = Mesh(mesh.devices.reshape(2, 4, 4, 2, 2), ALL)
    return jax.shard_map(
        shards,
        mesh=finer,
        in_specs=(P(ROW, COL), P(ROW, COL), P()),
        out_specs=(P(COL, ROW), P(COL, ROW), P(None, ROW)),
        check_vma=False,
    )
```
